32 devices in a mesh: band: 8 (over z, y), field: 4 (over x, core).
Axes of the slice: x: 2, y: 2, z: 4, core: 2. Of those that a mesh axis runs over, the one named last changes fastest.
Arguments:
- right_side: float32 [640, 2, 4, 12, 640], P('band', None, 'field'), may hold values from -40 to 40
- legendre: bfloat16 [640, 640, 640], P('band'), may hold values from -0.25 to 0.25
- wave_map: int32 [640], replicated, may hold values from 0 to 639, as said below
- obs_weight: float32 [640, 1280], P('band'), may hold values from 0.2 to 5
Outputs:
- solution: float32 [640, 2, 4, 12, 640], P('band', None, 'field')
- residual: float32 [640, 2, 4, 12, 640], P('band', None, 'field')
The draws below stay inside these ranges and needn't reach their ends.
Inputs may be any that keep to these rules, and one draw needn't show every extreme that they name: A permutation of 0 to 639; wave_map[s] lies in the same aligned block of 20 values as 639-s.
All inputs are finite; a program needn't handle non-finite values.
Results may differ from the reference program's by a relative error of at most 0.03.
Values may be sent and summed in bfloat16 or wider, within the bound.
A program may use at most 192 MiB of HBM per device.

```python
import math
import jax
import jax.numpy as jnp
from jax import lax

MW = 640
NLAT = 640
NLON = 1280
FIELDS = 4
LEV = 12
ITERS = 3


def draw_right_side(key, part):
    first_key, second_key = jax.random.split(key, 2)
    shape = (MW, 2, FIELDS, LEV, MW)
    base = jax.random.normal(first_key, shape, jnp.float32)
    scales = jnp.exp(jax.random.uniform(second_key, (1, 1, FIELDS, LEV, 1), jnp.float32, 0.0, math.log(10.0)))
    return jnp.clip(base * scales, -40.0, 40.0)


def shuffle_block(block_key):
    return jax.random.permutation(block_key, MW // 32)


def draw_wave_map(key, part):
    block_width = MW // 32
    subkeys = jax.random.split(key, 32)
    shuffled = jax.vmap(shuffle_block)(subkeys).astype(jnp.int32)
    starts = jnp.arange(32, dtype=jnp.int32)[:, None] * block_width
    return (MW - 1 - (starts + shuffled)).reshape(MW).astype(jnp.int32)


def steps_of(stream_key, extent, cuts, smallest, top_value):
    def one(axis_at, parts):
        draws = jax.random.uniform(jax.random.fold_in(jax.random.fold_in(stream_key, 6), axis_at), (parts,), jnp.float32, smallest / len(cuts), top_value / len(cuts))
        return jnp.repeat(jnp.exp(draws), extent[axis_at] // parts).reshape((-1,) + (1,) * (len(extent) - axis_at - 1))

    factor_of = one(*cuts[0])
    for cut in cuts[1:]:
        factor_of = factor_of * one(*cut)
    return factor_of


def centred(rng, shape, deviation, most, pieces=(), held_as=jnp.bfloat16):
    drawn = jax.random.normal(rng, shape, jnp.float32) * deviation
    if len(pieces) > 0:
        drawn = steps_of(rng, shape, pieces, -0.22, 0.18) * drawn
    return jnp.clip(drawn, min=-most, max=most).astype(held_as)


def setup_inputs(seed: int = 0) -> dict:
    splits = jax.random.split(jax.random.key(seed), 5)
    right_side = draw_right_side(jax.random.fold_in(splits[4], 71), 0)
    legendre = centred(splits[1], (MW, MW, NLAT), MW ** -0.5, 0.25, ((0, 8),))
    wave_map = draw_wave_map(jax.random.fold_in(splits[4], 71), 0)
    obs_weight = jnp.clip(jnp.exp(math.log(5.0) - 3.218876 * jax.random.uniform(splits[3], (NLAT, NLON), jnp.float32) ** steps_of(splits[3], (NLAT, NLON), ((0, 8),), -0.2, 0.2)), 0.2, 5.0)
    return {"right_side": right_side, "legendre": legendre, "wave_map": wave_map, "obs_weight": obs_weight}


def triangle_of(own_waves, degrees):
    return (jnp.arange(degrees, dtype=jnp.int32)[None, :] >= own_waves[:, None]).astype(jnp.float32)

def fourier_of(wave_map, lon_count):
    longitude = jnp.arange(lon_count, dtype=jnp.int32)
    phase_int = wave_map[:, None].astype(jnp.int32) * longitude[None, :] % lon_count
    angles = phase_int.astype(jnp.float32) * (2.0 * math.pi / lon_count)
    norm_factor = 1.0 / math.sqrt(wave_map.shape[0])
    return (jnp.stack([jnp.cos(angles), -jnp.sin(angles)], axis=1) * norm_factor).astype(jnp.bfloat16)

def operate(vector, legendre, fourier_table, triangle, obs_weight):
    masked_bf = (vector * triangle[:, None, None, None, :]).astype(jnp.bfloat16)
    coeffs = lax.dot_general(masked_bf, legendre, (((4,), (1,)), ((0,), (0,))), preferred_element_type=jnp.float32).astype(jnp.bfloat16)
    grid_vals = lax.dot_general(coeffs, fourier_table, (((0, 1), (0, 1)), ((), ())), preferred_element_type=jnp.float32)
    weighted = (grid_vals * obs_weight).astype(jnp.bfloat16)
    returned = lax.dot_general(fourier_table, weighted, (((2,), (3,)), ((), ())), preferred_element_type=jnp.float32).astype(jnp.bfloat16)
    adjoint = lax.dot_general(returned, legendre, (((4,), (2,)), ((0,), (0,))), preferred_element_type=jnp.float32)
    return vector + triangle[:, None, None, None, :] * adjoint

def reference(right_side, legendre, wave_map, obs_weight):
    triangle = triangle_of(wave_map, right_side.shape[4])
    fourier_table = fourier_of(wave_map, obs_weight.shape[1])
    residual = right_side * triangle[:, None, None, None, :]
    direction = residual
    solution = jnp.zeros_like(residual)
    norm_now = jnp.sum(residual * residual)
    for iteration in range(ITERS):
        image_vec = operate(direction, legendre, fourier_table, triangle, obs_weight)
        step_length = norm_now / jnp.sum(direction * image_vec)
        solution = solution + step_length * direction
        residual = residual - step_length * image_vec
        norm_next = jnp.sum(residual * residual)
        direction = residual + norm_next / norm_now * direction
        norm_now = norm_next
    return (solution, residual)
```

```python
import math

import jax
import jax.numpy as jnp
from jax import lax
from jax.sharding import PartitionSpec as P

ITERS = 3


def triangle_of(own_waves, degrees):
    return (jnp.arange(degrees, dtype=jnp.int32)[None, :] >= own_waves[:, None]).astype(jnp.float32)


def fourier_of(wave_map, lon_count):
    longitude = jnp.arange(lon_count, dtype=jnp.int32)
    phase_int = wave_map[:, None] * longitude[None, :] % lon_count
    angles = phase_int.astype(jnp.float32) * (2.0 * math.pi / lon_count)
    norm_factor = 1.0 / math.sqrt(wave_map.shape[0])
    return (jnp.stack([jnp.cos(angles), -jnp.sin(angles)], axis=1) * norm_factor).astype(
        jnp.bfloat16
    )


def grid_round(spread, fourier_flat, obs_weight):
    slots, parts, items, single, lat_rows = spread.shape
    flat = spread.reshape(slots * parts, items * single * lat_rows)
    grid_vals = lax.dot_general(
        flat, fourier_flat, (((0,), (0,)), ((), ())), preferred_element_type=jnp.float32
    )
    grid_vals = (
        grid_vals.reshape(items * single, lat_rows, fourier_flat.shape[1]) * obs_weight[None, :, :]
    )
    weighted = grid_vals.astype(jnp.bfloat16).reshape(
        items * single * lat_rows, fourier_flat.shape[1]
    )
    returned = lax.dot_general(
        fourier_flat, weighted, (((1,), (1,)), ((), ())), preferred_element_type=jnp.float32
    ).astype(jnp.bfloat16)
    return returned.reshape(slots, parts, items, single, lat_rows)


def legendre_back(returned, legendre):
    return lax.dot_general(
        returned, legendre, (((4,), (2,)), ((0,), (0,))), preferred_element_type=jnp.float32
    )


def paired_sums(residual, image_vec):
    return lax.psum(
        (jnp.sum(residual * residual), jnp.sum(residual * image_vec)), ("band", "field")
    )


def on_device(right_side, legendre, wave_map, obs_weight):
    slot_count = legendre.shape[0]
    band_count = lax.axis_size("band")
    lat_rows = obs_weight.shape[0]
    first_slot = lax.axis_index("band") * slot_count
    own_waves = lax.dynamic_slice_in_dim(wave_map, first_slot, slot_count)
    triangle = triangle_of(own_waves, right_side.shape[4])
    fourier_table = fourier_of(wave_map, obs_weight.shape[1])
    fourier_flat = fourier_table.reshape(2 * fourier_table.shape[0], fourier_table.shape[2])
    triangle_five = triangle[:, None, None, None, :]
    field_count = right_side.shape[2]
    level_count = right_side.shape[3]
    merged = field_count * level_count

    def operate(vector):
        masked_bf = (vector * triangle_five).astype(jnp.bfloat16)
        coeffs = lax.dot_general(
            masked_bf, legendre, (((4,), (1,)), ((0,), (0,))), preferred_element_type=jnp.float32
        ).astype(jnp.bfloat16)
        outgoing = coeffs.reshape(slot_count, 2, merged, band_count, lat_rows)
        spread = lax.all_to_all(outgoing, "band", split_axis=3, concat_axis=0, tiled=True)
        returned = grid_round(spread, fourier_flat, obs_weight)
        returned_home = lax.all_to_all(returned, "band", split_axis=0, concat_axis=3, tiled=True)
        home = returned_home.reshape(slot_count, 2, field_count, level_count, band_count * lat_rows)
        adjoint = legendre_back(home, legendre)
        return vector + triangle_five * adjoint

    residual = right_side * triangle_five
    solution = jnp.zeros_like(residual)
    image_vec = operate(residual)
    norm_now, product = paired_sums(residual, image_vec)
    step_length = norm_now / product
    direction = residual
    along = image_vec
    for iteration in range(ITERS):
        solution = solution + step_length * direction
        residual = residual - step_length * along
        if iteration + 1 < ITERS:
            image_vec = operate(residual)
            norm_next, product = paired_sums(residual, image_vec)
            beta_ratio = norm_next / norm_now
            step_length = norm_next / (product - beta_ratio * norm_next / step_length)
            direction = residual + beta_ratio * direction
            along = image_vec + beta_ratio * along
            norm_now = norm_next
    return (solution, residual)


LANES = 128


def tiled_split(levels, lat_count, band_count):
    tiles = lat_count // LANES
    return lat_count % LANES == 0 and tiles % 2 == 1 and 2 * levels == 3 * band_count


def fourier_phase(phase_int, lon_count, slot_total, part_axis):
    angles = phase_int.astype(jnp.float32) * (2.0 * math.pi / lon_count)
    norm_factor = 1.0 / math.sqrt(slot_total)
    return (jnp.stack([jnp.cos(angles), -jnp.sin(angles)], axis=part_axis) * norm_factor).astype(
        jnp.bfloat16
    )


def on_device_tiled(right_side, legendre, wave_map, obs_weight):
    slot_count, parts, field_count, level_count, degrees = right_side.shape
    band_count = lax.axis_size("band")
    levels = field_count * level_count
    lat_count = legendre.shape[2]
    lon_count = obs_weight.shape[1]
    slot_total = wave_map.shape[0]
    groups = band_count // 2
    shared = (lat_count // LANES + 1) // 2 * LANES
    width = lat_count + shared
    tail_from = lat_count - shared
    band_at = lax.axis_index("band")
    odd = band_at % 2
    own_waves = lax.dynamic_slice_in_dim(wave_map, band_at * slot_count, slot_count)
    triangle = triangle_of(own_waves, degrees)[:, None, :]

    longitude = jnp.arange(lon_count, dtype=jnp.int32)
    waves = wave_map.reshape(band_count, slot_count)
    rows_phase = waves[:, :, None] * longitude[None, None, :] % lon_count
    table = fourier_phase(rows_phase, lon_count, slot_total, 1)
    table = table.reshape(parts * slot_total, lon_count)
    cols_phase = longitude[:, None, None] * waves[None, :, :] % lon_count
    table_t = fourier_phase(cols_phase, lon_count, slot_total, 2)
    table_t = table_t.reshape(lon_count, parts * slot_total)
    table, table_t = lax.optimization_barrier((table, table_t))

    weight_all = lax.all_gather(obs_weight, "band", axis=0, tiled=True)
    weight_tail = lax.dynamic_slice_in_dim(weight_all, odd * tail_from, shared)
    weight_t = jnp.concatenate([weight_all, weight_tail], axis=0).T
    weight_t = lax.optimization_barrier(weight_t)
    column = jnp.arange(width, dtype=jnp.int32)
    twice = (column >= lat_count) & (column < lat_count + LANES) & (odd == 1)
    counted = jnp.where(twice, 0.0, 1.0).astype(jnp.float32)

    def operate(vector):
        masked_bf = (vector * triangle).astype(jnp.bfloat16)
        coeffs = lax.dot_general(
            masked_bf, legendre, (((2,), (1,)), ((0,), (0,))), preferred_element_type=jnp.float32
        ).astype(jnp.bfloat16)
        planes = coeffs.reshape(slot_count, parts, levels, lat_count).transpose(2, 1, 0, 3)
        planes = planes.reshape(groups, 3, parts * slot_count, lat_count)
        first = jnp.concatenate([planes[:, 0], planes[:, 1, :, :shared]], axis=2)
        second = jnp.concatenate([planes[:, 2], planes[:, 1, :, tail_from:]], axis=2)
        outgoing = jnp.stack([first, second], axis=1)
        outgoing = outgoing.reshape(band_count, parts * slot_count, width)
        spread = lax.all_to_all(outgoing, "band", split_axis=0, concat_axis=0, tiled=True)
        spread = spread.reshape(parts * slot_total, width)
        grid_t = lax.dot_general(
            table_t, spread, (((1,), (0,)), ((), ())), preferred_element_type=jnp.float32
        )
        weighted = grid_t * weight_t
        energy = jnp.sum(weighted * grid_t * counted[None, :])
        weighted_bf = weighted.astype(jnp.bfloat16)
        returned = lax.dot_general(
            table, weighted_bf, (((1,), (0,)), ((), ())), preferred_element_type=jnp.float32
        ).astype(jnp.bfloat16)
        returned = returned.reshape(band_count, parts * slot_count, width)
        sums = lax.psum((jnp.sum(vector * vector), energy), "field")
        norm, product = lax.psum(sums, "band")
        back = lax.all_to_all(returned, "band", split_axis=0, concat_axis=0, tiled=True)
        back = back.reshape(groups, 2, parts * slot_count, width)
        middle = jnp.concatenate(
            [back[:, 0, :, lat_count:], back[:, 1, :, lat_count + LANES :]], axis=2
        )
        home = jnp.stack([back[:, 0, :, :lat_count], middle, back[:, 1, :, :lat_count]], axis=1)
        home = home.reshape(levels, parts, slot_count, lat_count).transpose(2, 1, 0, 3)
        home = home.reshape(slot_count, parts * levels, lat_count)
        adjoint = lax.dot_general(
            home, legendre, (((2,), (2,)), ((0,), (0,))), preferred_element_type=jnp.float32
        )
        return vector + triangle * adjoint, norm, norm + product

    residual = right_side.reshape(slot_count, parts * levels, degrees) * triangle
    image_vec, norm_now, product = operate(residual)
    step_length = norm_now / product
    direction = residual
    along = image_vec
    solution = step_length * direction
    residual = residual - step_length * along
    for iteration in range(1, ITERS):
        image_vec, norm_next, product = operate(residual)
        beta_ratio = norm_next / norm_now
        step_length = norm_next / (product - beta_ratio * norm_next / step_length)
        direction = residual + beta_ratio * direction
        along = image_vec + beta_ratio * along
        norm_now = norm_next
        solution = solution + step_length * direction
        residual = residual - step_length * along
    return solution.reshape(right_side.shape), residual.reshape(right_side.shape)


def on_device_any(right_side, legendre, wave_map, obs_weight):
    levels = right_side.shape[2] * right_side.shape[3]
    if tiled_split(levels, legendre.shape[2], lax.axis_size("band")):
        return on_device_tiled(right_side, legendre, wave_map, obs_weight)
    return on_device(right_side, legendre, wave_map, obs_weight)


def solution(mesh):
    in_specs = (P("band", None, "field", None, None), P("band", None, None), P(), P("band", None))
    out_specs = (P("band", None, "field", None, None), P("band", None, "field", None, None))
    return jax.shard_map(
        on_device_any, mesh=mesh, in_specs=in_specs, out_specs=out_specs, check_vma=False
    )
```
